128 devices in a mesh: row: 8 (over y, core), col: 16 (over x, z).
Axes of the slice: x: 4, y: 4, z: 4, core: 2. Of those that a mesh axis runs over, the one named last changes fastest.
Arguments:
- measured: float32 [512, 128, 128], P(('row', 'col')), may hold values from 0 to 2
- positions: int32 [512, 2], P(('row', 'col')), may hold values from 0 to 1920, as said below
- probe: float32 [2, 128, 128], replicated, may hold values from -6 to 6
- prop_phase: float32 [128, 128], replicated, may hold values from -3.140625 to 3.140625
- object_real: float32 [4, 1024, 2048], P(None, 'row', 'col'), may hold values from 0.5 to 1.5
- object_imag: float32 [4, 1024, 2048], P(None, 'row', 'col'), may hold values from -1.8 to 1.8
Outputs:
- new_real: float32 [4, 1024, 2048], P(None, 'row', 'col')
- new_imag: float32 [4, 1024, 2048], P(None, 'row', 'col')
- new_probe: float32 [2, 128, 128], replicated
The draws below stay inside these ranges and needn't reach their ends.
Inputs may be any that keep to these rules, and one draw needn't show every extreme that they name: `positions`: frame f belongs to device d = f // 4, with r = d // 16 and c = d % 16. Its row lies from max(r * 128 - 64, 0) to min(r * 128 + 64, 896), both ends included; its column from max(c * 128 - 64, 0) to min(c * 128 + 64, 1920). On every device some frame takes the lower end and some frame the upper end of each of the two ranges.
All inputs are finite; a program needn't handle non-finite values.
Results may differ from the reference program's by a relative error of at most 0.0003.
Values sent between devices are 32-bit elements; how exact they have to be, the bound alone decides.
No kernel may reach another device: no remote copies, remote signals or barrier semaphores. Data moves between devices by JAX's collectives and lax.ppermute only.
A program may use at most 128 MiB of HBM per device.

```python
import jax
import jax.numpy as jnp
from jax import lax

PIX = 128
SLICES = 4
PASSES = 3
FR_DEV = 4
TILE_Y = 128
TILE_X = 128
HALF = 64
FRAMES = 512
OY = 1024
OX = 2048


def axis_positions(key, grid, tile, whole, local, device, devices):
    lower = jnp.maximum(grid * tile - HALF, 0)
    upper = jnp.minimum(grid * tile + tile - HALF, whole - PIX)
    span_count = upper - lower + 1
    key_raw, key_first, key_second = jax.random.split(key, 3)
    raw_draw = jax.random.randint(key_raw, (FRAMES,), 0, 1 << 20, dtype=jnp.int32) % span_count
    chosen = lower + raw_draw
    first_slot = jax.random.randint(key_first, (devices,), 0, FR_DEV, dtype=jnp.int32)
    second_slot = (first_slot + 1 + jax.random.randint(key_second, (devices,), 0, FR_DEV - 1, dtype=jnp.int32)) % FR_DEV
    chosen = jnp.where(local == first_slot[device], lower, chosen)
    chosen = jnp.where(local == second_slot[device], upper, chosen)
    return chosen


def draw_positions(key, part):
    devices = FRAMES // FR_DEV
    col_count = OX // TILE_X
    counter = jnp.arange(FRAMES, dtype=jnp.int32)
    device = counter // FR_DEV
    local = counter % FR_DEV
    row_grid = device // col_count
    col_grid = device % col_count
    row_pos = axis_positions(jax.random.fold_in(key, 11), row_grid, TILE_Y, OY, local, device, devices)
    col_pos = axis_positions(jax.random.fold_in(key, 12), col_grid, TILE_X, OX, local, device, devices)
    return jnp.stack((row_pos, col_pos), axis=1).astype(jnp.int32)


def shard_levels(own_key, dims, cuts, low, top_value):
    def one(dim, parts):
        draws = jax.random.uniform(jax.random.fold_in(jax.random.fold_in(own_key, 6), dim), (parts,), jnp.float32, low / len(cuts), top_value / len(cuts))
        return jnp.repeat(jnp.exp(draws), dims[dim] // parts).reshape((-1,) + (1,) * (len(dims) - dim - 1))

    gain = one(*cuts[0])
    for cut in cuts[1:]:
        gain = gain * one(*cut)
    return gain


def centred(own_key, dims, width, most, cuts=(), kind=jnp.bfloat16):
    result = width * jax.random.normal(own_key, dims, jnp.float32)
    if cuts:
        result = result * shard_levels(own_key, dims, cuts, -0.22, 0.18)
    return jnp.clip(result, -most, most).astype(kind)


def setup_inputs(seed: int = 0) -> dict:
    keys = jax.random.split(jax.random.key(seed), 7)
    return {
        "measured": jnp.clip(2.0 * jax.random.uniform(keys[0], (FRAMES, PIX, PIX), jnp.float32) ** shard_levels(keys[0], (FRAMES, PIX, PIX), ((0, 128),), -0.2, 0.2), 0.0, 2.0),
        "positions": draw_positions(jax.random.fold_in(keys[6], 71), 0),
        "probe": centred(keys[2], (2, PIX, PIX), 1.0, 6.0, (), jnp.float32),
        "prop_phase": jnp.clip(jax.random.uniform(keys[3], (PIX, PIX), jnp.float32, -3.140625, 3.140625), -3.140625, 3.140625),
        "object_real": jnp.clip(1.0 + 0.1 * jax.random.normal(keys[4], (SLICES, OY, OX), jnp.float32), 0.5, 1.5),
        "object_imag": centred(keys[5], (SLICES, OY, OX), 0.3, 1.8, ((1, 8), (2, 16)), jnp.float32),
    }


object_rate = 0.5
probe_rate = 0.5

def box_mean(field):
    padded = jnp.pad(field, ((0, 0), (1, 1), (1, 1)))
    row_count = field.shape[1]
    col_count = field.shape[2]
    summed = jnp.zeros_like(field)
    for row_at in range(3):
        for col_at in range(3):
            summed = summed + padded[:, row_at:row_at + row_count, col_at:col_at + col_count]
    return summed / 9.0

def reference(measured, positions, probe, prop_phase, object_real, object_imag):
    object_c = lax.complex(object_real, object_imag)
    probe_c = lax.complex(probe[0], probe[1])
    kernel = lax.complex(jnp.cos(prop_phase), jnp.sin(prop_phase))

    def one_frame(carry, inputs):
        object_grad, probe_grad = carry
        intensity, position = inputs
        zero_index = jnp.zeros((), jnp.int32)
        corner = (zero_index, position[0].astype(jnp.int32), position[1].astype(jnp.int32))
        transmit = lax.dynamic_slice(object_c, corner, (SLICES, PIX, PIX))
        waves = []
        wave = probe_c
        exit_wave = wave
        for slice_at in range(SLICES):
            waves.append(wave)
            exit_wave = wave * transmit[slice_at]
            if slice_at < SLICES - 1:
                wave = jnp.fft.ifft2(kernel * jnp.fft.fft2(exit_wave, norm='ortho'), norm='ortho')
        far_wave = jnp.fft.fft2(exit_wave, norm='ortho')
        residual = jnp.real(far_wave) ** 2 + jnp.imag(far_wave) ** 2 - intensity
        backward = jnp.fft.ifft2(residual * far_wave, norm='ortho')
        object_terms = [None] * SLICES
        probe_term = backward
        for slice_at in reversed(range(SLICES)):
            object_terms[slice_at] = jnp.conj(waves[slice_at]) * backward
            probe_term = jnp.conj(transmit[slice_at]) * backward
            if slice_at > 0:
                backward = jnp.fft.ifft2(jnp.conj(kernel) * jnp.fft.fft2(probe_term, norm='ortho'), norm='ortho')
        update = jnp.stack(object_terms)
        previous = lax.dynamic_slice(object_grad, corner, (SLICES, PIX, PIX))
        object_grad = lax.dynamic_update_slice(object_grad, previous + update, corner)
        return ((object_grad, probe_grad + probe_term), None)
    start = (jnp.zeros(object_c.shape, object_c.dtype), jnp.zeros(probe_c.shape, probe_c.dtype))
    (object_grad, probe_grad), _ = lax.scan(one_frame, start, (measured, positions))
    smooth_re = jnp.real(object_grad)
    smooth_im = jnp.imag(object_grad)
    for pass_at in range(PASSES):
        smooth_re = box_mean(smooth_re)
        smooth_im = box_mean(smooth_im)
    new_real = object_real - object_rate * smooth_re
    new_imag = object_imag - object_rate * smooth_im
    gradient = jnp.stack((jnp.real(probe_grad), jnp.imag(probe_grad)))
    norm_scale = jnp.sqrt(jnp.mean(gradient * gradient) + 1e-06)
    new_probe = probe - probe_rate * gradient / norm_scale
    return (new_real, new_imag, new_probe)
```

```python
import math

import numpy as np
import jax
import jax.numpy as jnp
from jax import lax
from jax.experimental import pallas as pl
from jax.experimental.pallas import tpu as pltpu
from jax.sharding import PartitionSpec as P

PIX = 128
HALF = 64
SL = 4
NP_ = 2 * SL
RIM = 72
F32 = jnp.float32
BF16 = jnp.bfloat16
AXES = ("row", "col")

object_rate = 0.5
probe_rate = 0.5


def dft_tables():
    counter = np.arange(PIX)
    angles = (counter[:, None] * counter[None, :] % PIX) * (2.0 * math.pi / PIX)
    cosine = np.cos(angles) / math.sqrt(PIX)
    sine = np.sin(angles) / math.sqrt(PIX)
    first = np.block([[cosine, -sine], [sine, cosine]]).astype(np.float32)
    high = np.asarray(first.astype(jnp.bfloat16))
    low = np.asarray((first - high.astype(np.float32)).astype(jnp.bfloat16))
    return np.stack([high, low, high.T, low.T])


def split(value):
    high = value.astype(BF16)
    low = (value - high.astype(F32)).astype(BF16)
    return high, low


def mm(left, right):
    return lax.dot_general(left, right, (((1,), (0,)), ((), ())), preferred_element_type=F32)


def mm_t(left, right):
    return lax.dot_general(left, right, (((1,), (1,)), ((), ())), preferred_element_type=F32)


def lane_of(shape):
    return lax.broadcasted_iota(jnp.int32, shape, 1)


def weights(delta):
    size = jnp.abs(delta)
    return jnp.where(
        size == 0, 7.0, jnp.where(size == 1, 6.0, jnp.where(size == 2, 3.0, jnp.where(size == 3, 1.0, 0.0)))
    ).astype(F32)


def smoothing(out_at, in_at, whole):
    inner = weights(out_at - in_at) - weights(out_at + in_at + 2) - weights(out_at + in_at - 2 * whole)
    return jnp.where(jnp.logical_and(out_at >= 0, out_at < whole), inner, 0.0)


def pack_kernel(real_ref, imag_ref, left_ref, right_ref):
    low = lane_of((HALF, PIX)) < HALF
    for plane in range(NP_):
        ref = real_ref if plane < SL else imag_ref
        top = ref[plane % SL, :HALF, :]
        bottom = ref[plane % SL, HALF:, :]
        left_ref[plane] = jnp.where(low, top, pltpu.roll(bottom, HALF, 1))
        right_ref[plane] = jnp.where(low, pltpu.roll(top, HALF, 1), bottom)


def join_kernel(real_ref, imag_ref, from_left_ref, from_right_ref, top_ref, bottom_ref):
    low = lane_of((HALF, PIX)) < HALF
    for plane in range(NP_):
        ref = real_ref if plane < SL else imag_ref
        for part, out_ref in ((0, top_ref), (1, bottom_ref)):
            own = pltpu.roll(ref[plane % SL, part * HALF : (part + 1) * HALF, :], HALF, 1)
            near = from_left_ref[plane]
            far = from_right_ref[plane]
            if part == 0:
                far = pltpu.roll(far, HALF, 1)
            else:
                near = pltpu.roll(near, HALF, 1)
            out_ref[plane, 0] = jnp.where(low, near, own)
            out_ref[plane, 1] = jnp.where(low, own, far)


def main_kernel(
    at_ref, up_ref, top_ref, bottom_ref, down_ref, measured_ref, probe_ref, kernel_ref, table_ref,
    up_out, down_out, mid_out, keep_out, send_out, window, patches, waves, grads,
):
    frames = measured_ref.shape[0]
    pairs = frames // 2
    for plane in range(NP_):
        for half in range(2):
            window[plane, half, 0:64] = up_ref[plane, half]
            window[plane, half, 64:128] = top_ref[plane, half]
            window[plane, half, 128:192] = bottom_ref[plane, half]
            window[plane, half, 192:256] = down_ref[plane, half]
    lane = lane_of((PIX, PIX))

    def cut(frame, slice_at):
        row_off = at_ref[2 * frame]
        col_off = at_ref[2 * frame + 1]
        turn = lax.rem(PIX - col_off, PIX)
        near = lane < PIX - col_off
        for plane in (slice_at, SL + slice_at):
            first = pltpu.roll(window[plane, 0, pl.ds(row_off, PIX), :], turn, 1)
            second = pltpu.roll(window[plane, 1, pl.ds(row_off, PIX), :], turn, 1)
            patches[frame, plane] = jnp.where(near, first, second)

    def right(pair, which):
        rows = [jnp.concatenate([re, im], axis=1) for re, im in pair]
        high, low = split(jnp.concatenate(rows, axis=0))
        table_high = table_ref[which]
        table_low = table_ref[which + 1]
        out = mm(high, table_high) + mm(high, table_low) + mm(low, table_high)
        return [(out[i * PIX : (i + 1) * PIX, :PIX], out[i * PIX : (i + 1) * PIX, PIX:]) for i in range(2)]

    def left(pair, which):
        value = jnp.concatenate(
            [jnp.concatenate([pair[0][k], pair[1][k]], axis=1) for k in range(2)], axis=0
        )
        high, low = split(value)
        table_high = table_ref[which]
        table_low = table_ref[which + 1]
        out = mm(table_high, high) + mm(table_low, high) + mm(table_high, low)
        return [(out[:PIX, i * PIX : (i + 1) * PIX], out[PIX:, i * PIX : (i + 1) * PIX]) for i in range(2)]

    def forward(items):
        items = [right(pair, 0) for pair in items]
        return [left(pair, 2) for pair in items]

    def inverse(items):
        items = [right(pair, 2) for pair in items]
        return [left(pair, 0) for pair in items]

    def each(items, fn):
        return [[fn(2 * p + i, *items[p][i]) for i in range(2)] for p in range(pairs)]

    def times(a_re, a_im, b_re, b_im):
        return a_re * b_re - a_im * b_im, a_re * b_im + a_im * b_re

    def conj_times(a_re, a_im, b_re, b_im):
        return a_re * b_re + a_im * b_im, a_re * b_im - a_im * b_re

    def through(frame, re, im):
        return times(kernel_ref[0], kernel_ref[1], re, im)

    def through_back(frame, re, im):
        return conj_times(kernel_ref[0], kernel_ref[1], re, im)

    def wave_of(frame, slice_at):
        if slice_at == 0:
            return probe_ref[0], probe_ref[1]
        return waves[slice_at - 1, frame, 0], waves[slice_at - 1, frame, 1]

    for slice_at in range(SL):
        for frame in range(frames):
            cut(frame, slice_at)

        def exit_of(frame, *unused, slice_at=slice_at):
            wave_re, wave_im = wave_of(frame, slice_at)
            return times(wave_re, wave_im, patches[frame, slice_at], patches[frame, SL + slice_at])

        items = each([[(), ()] for _ in range(pairs)], exit_of)
        items = forward(items)
        if slice_at < SL - 1:
            items = inverse(each(items, through))
            for p in range(pairs):
                for i in range(2):
                    waves[slice_at, 2 * p + i, 0] = items[p][i][0]
                    waves[slice_at, 2 * p + i, 1] = items[p][i][1]

    def residual_of(frame, re, im):
        residual = re * re + im * im - measured_ref[frame]
        return residual * re, residual * im

    back = inverse(each(items, residual_of))
    for slice_at in reversed(range(SL)):

        def emit(frame, re, im, slice_at=slice_at):
            wave_re, wave_im = wave_of(frame, slice_at)
            term_re, term_im = conj_times(wave_re, wave_im, re, im)
            grads[slice_at, frame] = term_re
            grads[SL + slice_at, frame] = term_im
            return conj_times(patches[frame, slice_at], patches[frame, SL + slice_at], re, im)

        back = each(back, emit)
        if slice_at > 0:
            back = inverse(each(forward(back), through_back))

    sums = []
    for k in range(2):
        total = back[0][0][k] + back[0][1][k]
        for p in range(1, pairs):
            total = total + (back[p][0][k] + back[p][1][k])
        sums.append(total)
    first_core = at_ref[8] == 0
    keep_out[...] = jnp.where(first_core, sums[0], sums[1])
    send_out[...] = jnp.where(first_core, sums[1], sums[0])

    row_base = at_ref[9]
    whole_rows = at_ref[10]
    shape = (256 + 16, PIX)
    out_at = lax.broadcasted_iota(jnp.int32, shape, 0) + (row_base - 8)
    in_at = lax.broadcasted_iota(jnp.int32, shape, 1) + row_base
    places = []
    for p in range(pairs):
        places.append(
            jnp.concatenate(
                [smoothing(out_at, in_at + at_ref[2 * (2 * p + i)], whole_rows) for i in range(2)], axis=1
            ).astype(BF16)
        )

    def place(plane, carry):
        out = None
        for p in range(pairs):
            rows = []
            for i in range(2):
                col_off = at_ref[2 * (2 * p + i) + 1]
                moved = pltpu.roll(grads[plane, 2 * p + i], lax.rem(col_off, PIX), 1)
                rows.append(
                    jnp.concatenate(
                        [jnp.where(lane >= col_off, moved, 0.0), jnp.where(lane < col_off, moved, 0.0)], axis=1
                    )
                )
            high, low = split(jnp.concatenate(rows, axis=0))
            part = mm(places[p], high) + mm(places[p], low)
            out = part if out is None else out + part
        for half in range(2):
            piece = out[:, half * PIX : (half + 1) * PIX]
            up_out[plane, half] = piece[0:RIM]
            mid_out[plane, half] = piece[RIM : RIM + PIX]
            down_out[plane, half] = piece[RIM + PIX :]
        return carry

    lax.fori_loop(0, NP_, place, 0)


def column_kernel(at_ref, mid_ref, from_up_ref, from_down_ref, left_out, right_out, center_out):
    col_base = at_ref[11]
    whole_cols = at_ref[12]
    shape = (256 + 16, 256)
    out_at = lax.broadcasted_iota(jnp.int32, shape, 0) + (col_base - 8)
    in_at = lax.broadcasted_iota(jnp.int32, shape, 1) + col_base
    table = smoothing(out_at, in_at, whole_cols).astype(BF16)
    for first in range(0, NP_, 2):
        rows = []
        for plane in (first, first + 1):
            halves = []
            for half in range(2):
                value = mid_ref[plane, half]
                add_top = from_up_ref[plane, half]
                add_low = from_down_ref[plane, half]
                halves.append(
                    jnp.concatenate(
                        [
                            value[:56] + add_top[:56],
                            value[56:RIM] + add_top[56:] + add_low[: RIM - 56],
                            value[RIM:] + add_low[RIM - 56 :],
                        ],
                        axis=0,
                    )
                )
            rows.append(jnp.concatenate(halves, axis=1))
        high, low = split(jnp.concatenate(rows, axis=0))
        out = mm_t(table, high) + mm_t(table, low)
        for i in range(2):
            piece = out[:, i * PIX : (i + 1) * PIX]
            left_out[first + i] = piece[0:RIM]
            center_out[first + i] = piece[RIM : RIM + PIX]
            right_out[first + i] = piece[RIM + PIX :]


def final_kernel(real_ref, imag_ref, center_ref, from_left_ref, from_right_ref, real_out, imag_out):
    scale = object_rate / 729.0
    for plane in range(NP_):
        value = center_ref[plane]
        add_low = from_left_ref[plane]
        add_high = from_right_ref[plane]
        total = jnp.concatenate(
            [
                value[:56] + add_low[:56],
                value[56:RIM] + add_low[56:] + add_high[: RIM - 56],
                value[RIM:] + add_high[RIM - 56 :],
            ],
            axis=0,
        )
        ref, out = (real_ref, real_out) if plane < SL else (imag_ref, imag_out)
        out[plane % SL] = ref[plane % SL] - scale * total.T


def probe_kernel(at_ref, own_ref, other_ref, probe_ref, out_ref):
    first_core = at_ref[8] == 0
    own = own_ref[...]
    other = other_ref[...]
    real = jnp.where(first_core, own, other)
    imag = jnp.where(first_core, other, own)
    mean = jnp.sum(real * real + imag * imag, keepdims=True) / (2.0 * PIX * PIX)
    scale = jnp.sqrt(mean + 1e-06)
    out_ref[0] = probe_ref[0] - probe_rate * real / scale
    out_ref[1] = probe_ref[1] - probe_rate * imag / scale


VMEM = pl.BlockSpec(memory_space=pltpu.VMEM)
SMEM = pl.BlockSpec(memory_space=pltpu.SMEM)


def call(fn, shapes, smem=0, scratch=(), flops=1_000_000):
    def run(*args):
        specs = [SMEM] * smem + [VMEM] * (len(args) - smem)
        return pl.pallas_call(
            fn,
            out_shape=[jax.ShapeDtypeStruct(s, F32) for s in shapes],
            in_specs=specs,
            out_specs=[VMEM] * len(shapes),
            scratch_shapes=list(scratch),
            cost_estimate=pl.CostEstimate(flops=flops, bytes_accessed=1_000_000, transcendentals=0),
            compiler_params=pltpu.CompilerParams(vmem_limit_bytes=60 * 1024 * 1024),
            name=fn.__name__,
        )(*args)

    return run


def turned(value, axis, by):
    count = lax.axis_size(axis)
    return lax.ppermute(value, axis, [(i, (i + by) % count) for i in range(count)])


def ring_of(axis, count, of, to):
    return [(i, to(i)) for i in range(count)]


def ring_total(value, axis, low, size):
    count = lax.axis_size(axis)

    def by(step):
        pairs = []
        for i in range(count):
            digit = i // low % size
            pairs.append((i, i + ((digit + step) % size - digit) * low))
        return lax.ppermute(value, axis, pairs)

    next_one, before, across = by(1), by(3), by(2)
    return (value + across) + (next_one + before)


def core_swap(value):
    count = lax.axis_size("row")
    return lax.ppermute(value, "row", [(i, i ^ 1) for i in range(count)])


def body(measured, positions, probe, prop_phase, object_real, object_imag):
    row_at = lax.axis_index("row")
    col_at = lax.axis_index("col")
    frames = measured.shape[0]
    base = jnp.stack([row_at * PIX - HALF, col_at * PIX - HALF]).astype(jnp.int32)
    offsets = (positions - base[None, :]).reshape(-1)
    extra = jnp.stack(
        [
            row_at % 2,
            base[0],
            jnp.int32(PIX * lax.axis_size("row")),
            base[1],
            jnp.int32(PIX * lax.axis_size("col")),
        ]
    ).astype(jnp.int32)
    at = jnp.concatenate([offsets, extra])

    face = (NP_, HALF, PIX)
    left_send, right_send = call(pack_kernel, [face, face])(object_real, object_imag)
    from_left = turned(right_send, "col", 1)
    from_right = turned(left_send, "col", -1)
    band = (NP_, 2, HALF, PIX)
    top, bottom = call(join_kernel, [band, band])(object_real, object_imag, from_left, from_right)
    up = turned(bottom, "row", 1)
    down = turned(top, "row", -1)
    kernel = jnp.stack([jnp.cos(prop_phase), jnp.sin(prop_phase)])
    tables = jnp.asarray(dft_tables())
    rim = (NP_, 2, RIM, PIX)
    flat = (PIX, PIX)
    up_send, down_send, middle, keep, send = call(
        main_kernel,
        [rim, rim, (NP_, 2, PIX, PIX), flat, flat],
        smem=1,
        scratch=[
            pltpu.VMEM((NP_, 2, 256, PIX), F32),
            pltpu.VMEM((frames, NP_, PIX, PIX), F32),
            pltpu.VMEM((SL - 1, frames, 2, PIX, PIX), F32),
            pltpu.VMEM((NP_, frames, PIX, PIX), F32),
        ],
        flops=12_000_000_000,
    )(at, up, top, bottom, down, measured, probe, kernel, tables)
    from_up = turned(down_send, "row", 1)
    from_down = turned(up_send, "row", -1)
    side = (NP_, RIM, PIX)
    left_out, right_out, center = call(column_kernel, [side, side, (NP_, PIX, PIX)], smem=1)(
        at, middle, from_up, from_down
    )
    side_left = turned(right_out, "col", 1)
    side_right = turned(left_out, "col", -1)
    tile = (SL, PIX, PIX)
    new_real, new_imag = call(final_kernel, [tile, tile])(
        object_real, object_imag, center, side_left, side_right
    )

    half_sum = keep + core_swap(send)
    half_sum = ring_total(half_sum, "col", 4, 4)
    half_sum = ring_total(half_sum, "col", 1, 4)
    half_sum = ring_total(half_sum, "row", 2, 4)
    other = core_swap(half_sum)
    (new_probe,) = call(probe_kernel, [(2, PIX, PIX)], smem=1)(at, half_sum, other, probe)
    return (new_real, new_imag, new_probe)


def solution(mesh):
    in_specs = (
        P(("row", "col"), None, None),
        P(("row", "col"), None),
        P(),
        P(),
        P(None, "row", "col"),
        P(None, "row", "col"),
    )
    out_specs = (P(None, "row", "col"), P(None, "row", "col"), P())
    return jax.shard_map(body, mesh=mesh, in_specs=in_specs, out_specs=out_specs, check_vma=False)
```
